32 devices in a mesh: dp: 4 (over z), mp: 8 (over y, x, core).
Axes of the slice: x: 2, y: 2, z: 4, core: 2. Of those that a mesh axis runs over, the one named last changes fastest.
Arguments:
- patches: bfloat16 [588, 768], P(None, ('dp', 'mp')), may hold values from -6 to 6
- embed_weight: bfloat16 [588, 6144], P(None, 'mp'), may hold values from -0.25 to 0.25
- embed_bias: float32 [6144], P('mp'), may hold values from -2 to 6
- pos_embed: bfloat16 [256, 6144], P(None, 'mp'), may hold values from -3 to 3
- norm_gain: float32 [6144], P('mp'), may hold values from 0.25 to 1.75
- inner_weight: bfloat16 [6144, 24576], P('dp', 'mp'), may hold values from -0.078125 to 0.078125
- inner_bias: float32 [24576], P('mp'), may hold values from -3 to 3
- outer_weight: bfloat16 [24576, 6144], P('mp', 'dp'), may hold values from -0.0546875 to 0.0546875
- outer_bias: float32 [6144], P('mp'), may hold values from -3 to 3
Outputs:
- block_out: float32 [768, 6144], P('dp', 'mp')
The draws below stay inside these ranges and needn't reach their ends.
All inputs are finite; a program needn't handle non-finite values.
Results may differ from the reference program's by a relative error of at most 0.006.
Values may be sent and summed in bfloat16 or wider, within the bound.
A program may use at most 192 MiB of HBM per device.

```python
import jax
import jax.numpy as jnp
from jax import lax

D = 6144
FF = 24576
PIX = 588
PATCHES = 256
TOKENS = 768
N_MP = 8


def draw_embed_bias(key, part):
    level_key = jax.random.fold_in(key, 11)
    noise_key = jax.random.fold_in(key, 12)
    block_of = jnp.arange(D, dtype=jnp.int32) * 64 // D
    levels = jax.random.uniform(level_key, (64,), jnp.float32, -1.0, 4.0)
    noise = jax.random.uniform(noise_key, (D,), jnp.float32, -1.0, 1.0)
    return (levels[block_of] + noise).astype(jnp.float32)


def strengthened(result, own_key, source, target, shards_of, factor):
    def block_of(position):
        return (jnp.arange(result.shape[position]) // (result.shape[position] // shards_of)).reshape((-1,) + (1,) * (result.ndim - 1 - position))

    one_side = jax.random.permutation(own_key, shards_of)[block_of(target)]
    second = (block_of(target) + shards_of // 2) % shards_of
    return jnp.where((block_of(source) == one_side) | (block_of(source) == second), factor * result, result)


def level_of(stream_key, shape, shards, least, high):
    def one(axis_at, blocks):
        heights = jax.random.uniform(jax.random.fold_in(jax.random.fold_in(stream_key, 6), axis_at), (blocks,), jnp.float32, least / len(shards), high / len(shards))
        return jnp.repeat(jnp.exp(heights), shape[axis_at] // blocks).reshape((-1,) + (1,) * (len(shape) - axis_at - 1))

    loudness = one(*shards[0])
    for cut in shards[1:]:
        loudness = loudness * one(*cut)
    return loudness


def normal_values(stream_key, shape, width, bound, shards=(), kind=jnp.bfloat16):
    gain = level_of(stream_key, shape, shards, -0.22, 0.18) if shards else 1.0
    entries = jax.random.normal(stream_key, shape, jnp.float32) * width * gain
    return jnp.minimum(jnp.maximum(entries, -bound), bound).astype(kind)


def gaussian_with(own_key, extent, deviation, most, cuts, heavy, held_as=jnp.bfloat16):
    entries = deviation * jax.random.normal(own_key, extent, jnp.float32)
    if cuts:
        entries = entries * level_of(own_key, extent, cuts, -0.22, 0.18)
    return jnp.clip(strengthened(entries, jax.random.fold_in(own_key, 3), *heavy), -most, most).astype(held_as)


def setup_inputs(seed: int = 0) -> dict:
    seeds = jax.random.split(jax.random.key(seed), 10)
    return {
        "patches": normal_values(seeds[0], (PIX, TOKENS), 1.0, 6.0, ((1, 32),)),
        "embed_weight": normal_values(seeds[1], (PIX, D), PIX ** -0.5, 0.25, ((1, 8),)),
        "embed_bias": draw_embed_bias(jax.random.fold_in(seeds[9], 71), 0),
        "pos_embed": normal_values(seeds[3], (PATCHES, D), 0.5, 3.0, ((1, 8),)),
        "norm_gain": jnp.clip(1.0 + 0.15 * jax.random.normal(seeds[4], (D,), jnp.float32), 0.25, 1.75),
        "inner_weight": normal_values(seeds[5], (D, FF), D ** -0.5, 0.078125, ((0, 4), (1, 8))),
        "inner_bias": normal_values(seeds[6], (FF,), 0.5, 3.0, ((0, 8),), jnp.float32),
        "outer_weight": gaussian_with(seeds[7], (FF, D), FF ** -0.5, 0.0546875, ((0, 8), (1, 4)), (0, 1, 8, 2.0)),
        "outer_bias": normal_values(seeds[8], (D,), 0.5, 3.0, ((0, 8),), jnp.float32),
    }


norm_eps = 1e-06

def reference(patches, embed_weight, embed_bias, pos_embed, norm_gain, inner_weight, inner_bias, outer_weight, outer_bias):
    product = jnp.dot(patches.T, embed_weight, preferred_element_type=jnp.float32)
    table = jnp.tile(pos_embed.astype(jnp.float32), (TOKENS // PATCHES, 1))
    embedded = product + embed_bias[None, :] + table
    row_mean = lax.optimization_barrier(jnp.sum(embedded, axis=1, keepdims=True)) / D
    centred = embedded - row_mean
    row_var = lax.optimization_barrier(jnp.sum(centred * centred, axis=1, keepdims=True)) / D
    normed = (centred * lax.rsqrt(row_var + norm_eps) * norm_gain[None, :]).astype(jnp.bfloat16)
    preact = jnp.dot(normed, inner_weight, preferred_element_type=jnp.float32) + inner_bias[None, :]
    hidden = jax.nn.gelu(preact, approximate=False).astype(jnp.bfloat16)
    block_width = FF // N_MP

    def add_block(block_index, running):
        begin_at = (block_index * block_width).astype(jnp.int32)
        hidden_cols = lax.dynamic_slice_in_dim(hidden, begin_at, block_width, 1)
        weight_rows = lax.dynamic_slice_in_dim(outer_weight, begin_at, block_width, 0)
        partial_k = jnp.dot(hidden_cols, weight_rows, preferred_element_type=jnp.float32).astype(jnp.bfloat16)
        partial_k = lax.optimization_barrier(partial_k)
        return running + partial_k.astype(jnp.float32)
    summed = lax.fori_loop(jnp.int32(0), jnp.int32(N_MP), add_block, jnp.zeros((TOKENS, D), jnp.float32))
    return embedded + summed + outer_bias[None, :]
```

```python
import jax
import jax.numpy as jnp
from jax import lax
from jax.sharding import PartitionSpec as P

norm_eps = 1e-06


def contract_first(left, right):
    return lax.dot_general(
        left, right, (((0,), (0,)), ((), ())), preferred_element_type=jnp.float32
    )


def per_device(
    patches,
    embed_weight,
    embed_bias,
    pos_embed,
    norm_gain,
    inner_weight,
    inner_bias,
    outer_weight,
    outer_bias,
):
    n_dp = lax.axis_size("dp")
    n_mp = lax.axis_size("mp")
    ratio = n_mp // n_dp
    group_rows = patches.shape[1] * n_mp
    width = embed_weight.shape[1]
    model_width = width * n_mp
    n_positions = pos_embed.shape[0]
    first_row = lax.axis_index("dp") * group_rows
    positions = (first_row + jnp.arange(group_rows, dtype=jnp.int32)) % n_positions
    selector = (positions[:, None] == jnp.arange(n_positions, dtype=jnp.int32)[None, :]).astype(
        jnp.bfloat16
    )
    all_patches = lax.all_gather(patches, "mp", axis=1, tiled=True)
    product = contract_first(all_patches, embed_weight)
    residual = product + embed_bias[None, :]
    residual = residual + jnp.dot(selector, pos_embed, preferred_element_type=jnp.float32)
    row_total = lax.psum(jnp.sum(residual, axis=1), "mp")
    row_mean = row_total / model_width
    centred = residual - row_mean[:, None]
    row_var = lax.psum(jnp.sum(centred * centred, axis=1), "mp") / model_width
    normed = (centred * lax.rsqrt(row_var + norm_eps)[:, None] * norm_gain[None, :]).astype(
        jnp.bfloat16
    )

    there = []
    for r in range(n_dp):
        for c in range(n_mp):
            there.append((r * n_mp + c, (c // ratio) * n_mp + r * ratio + c % ratio))
    back = [(b, a) for a, b in there]
    moved = lax.ppermute(normed, ("dp", "mp"), there)
    blocks = lax.all_gather(moved, "mp", axis=0, tiled=False)
    own_rows = (
        blocks.reshape(n_dp, ratio, group_rows, width)
        .transpose(0, 2, 1, 3)
        .reshape(n_dp * group_rows, ratio * width)
    )
    preact_part = jnp.dot(own_rows, inner_weight, preferred_element_type=jnp.float32)
    preact = lax.psum_scatter(
        preact_part.astype(jnp.bfloat16), "dp", scatter_dimension=0, tiled=True
    ).astype(jnp.float32)
    hidden = jax.nn.gelu(preact + inner_bias[None, :], approximate=False).astype(jnp.bfloat16)
    all_hidden = lax.all_gather(hidden, "dp", axis=0, tiled=True)
    partials = jnp.dot(all_hidden, outer_weight, preferred_element_type=jnp.float32).astype(
        jnp.bfloat16
    )
    partials = (
        partials.reshape(n_dp, group_rows, ratio, width)
        .transpose(0, 2, 1, 3)
        .reshape(n_mp * group_rows, width)
    )
    summed = lax.psum_scatter(partials, "mp", scatter_dimension=0, tiled=True)
    mlp_out = lax.ppermute(summed, ("dp", "mp"), back).astype(jnp.float32)
    return residual + mlp_out + outer_bias[None, :]


def solution(mesh):
    placed = (
        P(None, ("dp", "mp")),
        P(None, "mp"),
        P("mp"),
        P(None, "mp"),
        P("mp"),
        P("dp", "mp"),
        P("mp"),
        P("mp", "dp"),
        P("mp"),
    )
    return jax.shard_map(
        per_device, mesh=mesh, in_specs=placed, out_specs=P("dp", "mp"), check_vma=False
    )
```

```python
import functools

import jax
import jax.numpy as jnp
from jax import lax
from jax.experimental import pallas as pl
from jax.experimental.pallas import tpu as pltpu
from jax.sharding import PartitionSpec as P

norm_eps = 1e-06


def contract_first(left, right):
    return lax.dot_general(
        left, right, (((0,), (0,)), ((), ())), preferred_element_type=jnp.float32
    )

LANES = 128


def line_kernel(n, part, bias, out, from_left, from_right, send_sems, left_sems, right_sems, block_sems):
    z = lax.axis_index("dp")
    total, columns = part.shape
    rows = total // n
    chunks = columns // LANES
    settled = [max(k, n - 1 - k) for k in range(n)]
    steps = chunks + max(settled[o] + abs(k - o) for o in range(n) for k in range(n))

    def at(ref, first, last, c):
        lanes = pl.ds(pl.multiple_of(c * LANES, LANES), LANES)
        return ref.at[pl.ds(first * rows, (last - first) * rows), lanes]

    def send(src, dst, send_sem, recv_sem, to):
        return pltpu.make_async_remote_copy(
            src_ref=src,
            dst_ref=dst,
            send_sem=send_sem,
            recv_sem=recv_sem,
            device_id={"dp": to},
            device_id_type=pl.DeviceIdType.MESH,
        )

    barrier = pltpu.get_barrier_semaphore()
    for k in range(n):

        @pl.when(z == k)
        def _(k=k):
            near = [o for o in (k - 1, k + 1) if 0 <= o < n]
            for o in near:
                pl.semaphore_signal(
                    barrier, inc=1, device_id={"dp": o}, device_id_type=pl.DeviceIdType.MESH
                )
            pl.semaphore_wait(barrier, len(near))

    def role(k):
        has_left, has_right = k > 0, k < n - 1

        def wait_left(c):
            at_c = at(from_left, k, n, c)
            send(at_c, at_c, send_sems.at[0], left_sems.at[c], k - 1).wait_recv()

        def wait_right(c):
            at_c = at(from_right, 0, k + 1, c)
            send(at_c, at_c, send_sems.at[1], right_sems.at[c], k + 1).wait_recv()

        def add_own(ref, first, last, c):
            held = at(ref, first, last, c)
            own = at(part, first, last, c)
            held[...] = (held[...].astype(jnp.float32) + own[...].astype(jnp.float32)).astype(
                jnp.bfloat16
            )

        def pass_right(c):
            src = part
            if has_left:
                wait_left(c)
                add_own(from_left, k + 1, n, c)
                src = from_left
            send(
                at(src, k + 1, n, c),
                at(from_left, k + 1, n, c),
                send_sems.at[0],
                left_sems.at[c],
                k + 1,
            ).start()

        def pass_left(c):
            src = part
            if has_right:
                wait_right(c)
                add_own(from_right, 0, k, c)
                src = from_right
            send(
                at(src, 0, k, c),
                at(from_right, 0, k, c),
                send_sems.at[1],
                right_sems.at[c],
                k - 1,
            ).start()

        def give(c, origin, to):
            block = at(out, origin, origin + 1, c)
            sem = send_sems.at[2] if to > k else send_sems.at[3]
            return send(block, block, sem, block_sems.at[origin, c], to)

        def settle(c):
            if not has_right:
                wait_left(c)
            if not has_left:
                wait_right(c)
            x = at(part, k, k + 1, c)[...].astype(jnp.float32)
            if has_left:
                x = x + at(from_left, k, k + 1, c)[...].astype(jnp.float32)
            if has_right:
                x = x + at(from_right, k, k + 1, c)[...].astype(jnp.float32)
            x = x + bias[:, pl.ds(pl.multiple_of(c * LANES, LANES), LANES)]
            x = 0.5 * x * (1.0 + lax.erf(x * (0.5**0.5)))
            at(out, k, k + 1, c)[...] = x.astype(jnp.bfloat16)
            if has_right:
                give(c, k, k + 1).start()
            if has_left:
                give(c, k, k - 1).start()

        def relay(origin, c):
            give(c, origin, k - 1 if origin < k else k + 1).wait_recv()
            to = k + 1 if origin < k else k - 1
            if 0 <= to < n:
                give(c, origin, to).start()

        def run(c, action):
            @pl.when(jnp.logical_and(c >= 0, c < chunks))
            def _():
                action(c)

        def step(s, carry):
            if has_right:
                run(s - k, pass_right)
            if has_left:
                run(s - (n - 1 - k), pass_left)
            run(s - settled[k], settle)
            for origin in sorted((o for o in range(n) if o != k), key=lambda o: -abs(o - k)):
                run(s - settled[origin] - abs(origin - k), functools.partial(relay, origin))
            return carry

        lax.fori_loop(0, steps, step, 0)

        def drain(ref, first, last, sem, to):
            sent = ref.at[pl.ds(first * rows, (last - first) * rows), :]
            send(sent, sent, sem, block_sems.at[0, 0], to).wait_send()

        if has_right:
            drain(part, k + 1, n, send_sems.at[0], k + 1)
            drain(out, 0, k + 1, send_sems.at[2], k + 1)
        if has_left:
            drain(part, 0, k, send_sems.at[1], k - 1)
            drain(out, k, n, send_sems.at[3], k - 1)

    for k in range(n):
        pl.when(z == k)(functools.partial(role, k))


def hidden_of(n, part, bias):
    total, columns = part.shape
    chunks = columns // LANES
    vmem = pl.BlockSpec(memory_space=pltpu.VMEM)
    return pl.pallas_call(
        functools.partial(line_kernel, n),
        out_shape=jax.ShapeDtypeStruct(part.shape, jnp.bfloat16),
        in_specs=[vmem, vmem],
        out_specs=vmem,
        scratch_shapes=[
            pltpu.VMEM(part.shape, jnp.bfloat16),
            pltpu.VMEM(part.shape, jnp.bfloat16),
            pltpu.SemaphoreType.DMA((4,)),
            pltpu.SemaphoreType.DMA((chunks,)),
            pltpu.SemaphoreType.DMA((chunks,)),
            pltpu.SemaphoreType.DMA((n, chunks)),
        ],
        compiler_params=pltpu.CompilerParams(
            collective_id=0, has_side_effects=True, vmem_limit_bytes=40 * 1024 * 1024
        ),
    )(part, bias)


def per_device(
    patches,
    embed_weight,
    embed_bias,
    pos_embed,
    norm_gain,
    inner_weight,
    inner_bias,
    outer_weight,
    outer_bias,
):
    n_dp = lax.axis_size("dp")
    n_mp = lax.axis_size("mp")
    ratio = n_mp // n_dp
    group_rows = patches.shape[1] * n_mp
    width = embed_weight.shape[1]
    model_width = width * n_mp
    n_positions = pos_embed.shape[0]
    first_row = lax.axis_index("dp") * group_rows
    positions = (first_row + jnp.arange(group_rows, dtype=jnp.int32)) % n_positions
    selector = (positions[:, None] == jnp.arange(n_positions, dtype=jnp.int32)[None, :]).astype(
        jnp.bfloat16
    )
    all_patches = lax.all_gather(patches, "mp", axis=1, tiled=True)
    product = contract_first(all_patches, embed_weight)
    residual = product + embed_bias[None, :]
    residual = residual + jnp.dot(selector, pos_embed, preferred_element_type=jnp.float32)
    row_total = lax.psum(jnp.sum(residual, axis=1), "mp")
    row_mean = row_total / model_width
    centred = residual - row_mean[:, None]
    row_var = lax.psum(jnp.sum(centred * centred, axis=1), "mp") / model_width
    normed = (centred * lax.rsqrt(row_var + norm_eps)[:, None] * norm_gain[None, :]).astype(
        jnp.bfloat16
    )

    there = []
    for r in range(n_dp):
        for c in range(n_mp):
            there.append((r * n_mp + c, (c // ratio) * n_mp + r * ratio + c % ratio))
    back = [(b, a) for a, b in there]
    moved = lax.ppermute(normed, ("dp", "mp"), there)
    blocks = lax.all_gather(moved, "mp", axis=0, tiled=False)
    own_rows = (
        blocks.reshape(n_dp, ratio, group_rows, width)
        .transpose(0, 2, 1, 3)
        .reshape(n_dp * group_rows, ratio * width)
    )
    preact_part = jnp.dot(own_rows, inner_weight, preferred_element_type=jnp.float32)
    all_hidden = hidden_of(n_dp, preact_part.astype(jnp.bfloat16), inner_bias[None, :])
    partials = jnp.dot(all_hidden, outer_weight, preferred_element_type=jnp.float32).astype(
        jnp.bfloat16
    )
    partials = (
        partials.reshape(n_dp, group_rows, ratio, width)
        .transpose(0, 2, 1, 3)
        .reshape(n_mp * group_rows, width)
    )
    summed = lax.psum_scatter(partials, "mp", scatter_dimension=0, tiled=True)
    mlp_out = lax.ppermute(summed, ("dp", "mp"), back).astype(jnp.float32)
    return residual + mlp_out + outer_bias[None, :]


def solution(mesh):
    placed = (
        P(None, ("dp", "mp")),
        P(None, "mp"),
        P("mp"),
        P(None, "mp"),
        P("mp"),
        P("dp", "mp"),
        P("mp"),
        P("mp", "dp"),
        P("mp"),
    )
    return jax.shard_map(
        per_device, mesh=mesh, in_specs=placed, out_specs=P("dp", "mp"), check_vma=False
    )
```

```python
import functools

import jax
import jax.numpy as jnp
from jax import lax
from jax.experimental import pallas as pl
from jax.experimental.pallas import tpu as pltpu
from jax.sharding import PartitionSpec as P

norm_eps = 1e-06


def contract_first(left, right):
    return lax.dot_general(
        left, right, (((0,), (0,)), ((), ())), preferred_element_type=jnp.float32
    )

LANES = 128


def line_kernel(n, part, bias, out, from_left, from_right, send_sems, left_sems, right_sems, block_sems):
    z = lax.axis_index("dp")
    total, columns = part.shape
    rows = total // n
    chunks = columns // LANES
    settled = [max(k, n - 1 - k) for k in range(n)]
    steps = chunks + max(settled[o] + abs(k - o) for o in range(n) for k in range(n))

    def at(ref, first, last, c):
        lanes = pl.ds(pl.multiple_of(c * LANES, LANES), LANES)
        return ref.at[pl.ds(first * rows, (last - first) * rows), lanes]

    def send(src, dst, send_sem, recv_sem, to):
        return pltpu.make_async_remote_copy(
            src_ref=src,
            dst_ref=dst,
            send_sem=send_sem,
            recv_sem=recv_sem,
            device_id={"dp": to},
            device_id_type=pl.DeviceIdType.MESH,
        )

    barrier = pltpu.get_barrier_semaphore()
    for k in range(n):

        @pl.when(z == k)
        def _(k=k):
            near = [o for o in (k - 1, k + 1) if 0 <= o < n]
            for o in near:
                pl.semaphore_signal(
                    barrier, inc=1, device_id={"dp": o}, device_id_type=pl.DeviceIdType.MESH
                )
            pl.semaphore_wait(barrier, len(near))

    def role(k):
        has_left, has_right = k > 0, k < n - 1

        def wait_left(c):
            at_c = at(from_left, k, n, c)
            send(at_c, at_c, send_sems.at[0], left_sems.at[c], k - 1).wait_recv()

        def wait_right(c):
            at_c = at(from_right, 0, k + 1, c)
            send(at_c, at_c, send_sems.at[1], right_sems.at[c], k + 1).wait_recv()

        def add_own(ref, first, last, c):
            held = at(ref, first, last, c)
            own = at(part, first, last, c)
            held[...] = (held[...].astype(jnp.float32) + own[...].astype(jnp.float32)).astype(
                jnp.bfloat16
            )

        def pass_right(c):
            src = part
            if has_left:
                wait_left(c)
                add_own(from_left, k + 1, n, c)
                src = from_left
            send(
                at(src, k + 1, n, c),
                at(from_left, k + 1, n, c),
                send_sems.at[0],
                left_sems.at[c],
                k + 1,
            ).start()

        def pass_left(c):
            src = part
            if has_right:
                wait_right(c)
                add_own(from_right, 0, k, c)
                src = from_right
            send(
                at(src, 0, k, c),
                at(from_right, 0, k, c),
                send_sems.at[1],
                right_sems.at[c],
                k - 1,
            ).start()

        def give(c, origin, to):
            block = at(out, origin, origin + 1, c)
            sem = send_sems.at[2] if to > k else send_sems.at[3]
            return send(block, block, sem, block_sems.at[origin, c], to)

        def settle(c):
            if not has_right:
                wait_left(c)
            if not has_left:
                wait_right(c)
            x = at(part, k, k + 1, c)[...].astype(jnp.float32)
            if has_left:
                x = x + at(from_left, k, k + 1, c)[...].astype(jnp.float32)
            if has_right:
                x = x + at(from_right, k, k + 1, c)[...].astype(jnp.float32)
            x = x + bias[:, pl.ds(pl.multiple_of(c * LANES, LANES), LANES)]
            x = 0.5 * x * (1.0 + lax.erf(x * (0.5**0.5)))
            at(out, k, k + 1, c)[...] = x.astype(jnp.bfloat16)
            if has_right:
                give(c, k, k + 1).start()
            if has_left:
                give(c, k, k - 1).start()

        def relay(origin, c):
            give(c, origin, k - 1 if origin < k else k + 1).wait_recv()
            to = k + 1 if origin < k else k - 1
            if 0 <= to < n:
                give(c, origin, to).start()

        def run(c, action):
            @pl.when(jnp.logical_and(c >= 0, c < chunks))
            def _():
                action(c)

        def step(s, carry):
            if has_right:
                run(s - k, pass_right)
            if has_left:
                run(s - (n - 1 - k), pass_left)
            run(s - settled[k], settle)
            for origin in sorted((o for o in range(n) if o != k), key=lambda o: -abs(o - k)):
                run(s - settled[origin] - abs(origin - k), functools.partial(relay, origin))
            return carry

        lax.fori_loop(0, steps, step, 0)

        def drain(ref, first, last, sem, to):
            sent = ref.at[pl.ds(first * rows, (last - first) * rows), :]
            send(sent, sent, sem, block_sems.at[0, 0], to).wait_send()

        if has_right:
            drain(part, k + 1, n, send_sems.at[0], k + 1)
            drain(out, 0, k + 1, send_sems.at[2], k + 1)
        if has_left:
            drain(part, 0, k, send_sems.at[1], k - 1)
            drain(out, k, n, send_sems.at[3], k - 1)

    for k in range(n):
        pl.when(z == k)(functools.partial(role, k))


def hidden_of(n, part, bias):
    total, columns = part.shape
    chunks = columns // LANES
    vmem = pl.BlockSpec(memory_space=pltpu.VMEM)
    return pl.pallas_call(
        functools.partial(line_kernel, n),
        out_shape=jax.ShapeDtypeStruct(part.shape, jnp.bfloat16),
        in_specs=[vmem, vmem],
        out_specs=vmem,
        scratch_shapes=[
            pltpu.VMEM(part.shape, jnp.bfloat16),
            pltpu.VMEM(part.shape, jnp.bfloat16),
            pltpu.SemaphoreType.DMA((4,)),
            pltpu.SemaphoreType.DMA((chunks,)),
            pltpu.SemaphoreType.DMA((chunks,)),
            pltpu.SemaphoreType.DMA((n, chunks)),
        ],
        compiler_params=pltpu.CompilerParams(
            collective_id=0, has_side_effects=True, vmem_limit_bytes=40 * 1024 * 1024
        ),
    )(part, bias)

PIECES = 4
MESH = pl.DeviceIdType.MESH


def places(n, ratio):
    i, m = lax.axis_index("dp"), lax.axis_index("mp")
    parity = lax.rem(m, 2)
    other = {"mp": m + 1 - 2 * parity}
    mirror = {"dp": m // ratio, "mp": i * ratio + lax.rem(m, ratio)}
    alone = jnp.logical_and(m // ratio == i, i * ratio + lax.rem(m, ratio) == m)
    return m, parity, other, mirror, alone


def slot_of(n, ratio, m):
    return lax.rem(m, ratio) * n + m // ratio


def greet(chips, m, parity, other, mirror, alone):
    barrier = pltpu.get_barrier_semaphore()
    pl.semaphore_signal(barrier, inc=1, device_id=other, device_id_type=MESH)

    def call(j, carry):
        mate = 2 * lax.rem(m // 2 + j, chips) + parity
        pl.semaphore_signal(barrier, inc=1, device_id={"mp": mate}, device_id_type=MESH)
        return carry

    lax.fori_loop(1, chips, call, 0)

    @pl.when(jnp.logical_not(alone))
    def _():
        pl.semaphore_signal(barrier, inc=1, device_id=mirror, device_id_type=MESH)
        pl.semaphore_wait(barrier, chips + 1)

    @pl.when(alone)
    def _():
        pl.semaphore_wait(barrier, chips)


def push(src, dst, send_sem, recv_sem, to):
    return pltpu.make_async_remote_copy(
        src_ref=src,
        dst_ref=dst,
        send_sem=send_sem,
        recv_sem=recv_sem,
        device_id=to,
        device_id_type=MESH,
    )


def gather_kernel(n, ratio, own, out, send_sems, held_sems, block_sems):
    m, parity, other, mirror, alone = places(n, ratio)
    members, rows, _ = out.shape
    chips = members // 2
    tall = rows // PIECES
    held = slot_of(n, ratio, m)
    target = slot_of(n, ratio, mirror["mp"])
    greet(chips, m, parity, other, mirror, alone)

    def piece(slot, s):
        return out.at[slot, pl.ds(s * tall, tall)]

    def first(s):
        return push(
            own.at[pl.ds(s * tall, tall)], piece(target, s), send_sems.at[0], held_sems.at[s], mirror
        )

    @pl.when(jnp.logical_not(alone))
    def _():
        for s in range(PIECES):
            first(s).start()

    @pl.when(alone)
    def _():
        out[held] = own[...]

    def share(slot, sender, s, to):
        block = piece(slot, s)
        return push(block, block, send_sems.at[1], block_sems.at[sender, s], to)

    for s in range(PIECES):

        @pl.when(jnp.logical_not(alone))
        def _(s=s):
            push(piece(held, s), piece(held, s), send_sems.at[0], held_sems.at[s], mirror).wait_recv()

        def spread(j, carry, s=s):
            share(held, m, s, {"mp": 2 * lax.rem(m // 2 + j, chips) + parity}).start()
            return carry

        lax.fori_loop(1, chips, spread, 0)
        share(held, m, s, other).start()

    for s in range(PIECES):

        def forward(j, carry, s=s):
            sender = 2 * lax.rem(m // 2 + j, chips) + parity
            copy = share(slot_of(n, ratio, sender), sender, s, other)
            copy.wait_recv()
            copy.start()
            return carry

        lax.fori_loop(1, chips, forward, 0)

    for s in range(PIECES):

        def arrive(j, carry, s=s):
            sender = 2 * lax.rem(m // 2 + j, chips) + 1 - parity
            share(slot_of(n, ratio, sender), sender, s, other).wait_recv()
            return carry

        lax.fori_loop(0, chips, arrive, 0)

    @pl.when(jnp.logical_not(alone))
    def _():
        push(own, own, send_sems.at[0], held_sems.at[0], mirror).wait_send()

    sent = out.at[pl.ds(0, members - 1)]
    push(sent, sent, send_sems.at[1], held_sems.at[0], other).wait_send()


def blocks_of(n, members, own):
    vmem = pl.BlockSpec(memory_space=pltpu.VMEM)
    return pl.pallas_call(
        functools.partial(gather_kernel, n, members // n),
        out_shape=jax.ShapeDtypeStruct((members,) + own.shape, jnp.bfloat16),
        in_specs=[vmem],
        out_specs=vmem,
        scratch_shapes=[
            pltpu.SemaphoreType.DMA((2,)),
            pltpu.SemaphoreType.DMA((PIECES,)),
            pltpu.SemaphoreType.DMA((members, PIECES)),
        ],
        compiler_params=pltpu.CompilerParams(
            collective_id=1, has_side_effects=True, vmem_limit_bytes=40 * 1024 * 1024
        ),
    )(own)


def scatter_kernel(
    n, ratio, parts, out, pair_in, plane_in, done, send_sems, pair_sems, plane_sems, out_sems
):
    m, parity, other, mirror, alone = places(n, ratio)
    members, rows, _ = parts.shape
    chips = members // 2
    tall = rows // PIECES
    here = m // 2
    greet(chips, m, parity, other, mirror, alone)

    def lines(s):
        return pl.ds(s * tall, tall)

    def own_part(chip, side, s):
        return parts.at[slot_of(n, ratio, 2 * chip + side), lines(s)]

    def to_pair(chip, s):
        return push(
            own_part(chip, 1 - parity, s),
            pair_in.at[chip, lines(s)],
            send_sems.at[0],
            pair_sems.at[chip, s],
            other,
        )

    def to_plane(chip, s):
        return push(
            pair_in.at[chip, lines(s)],
            plane_in.at[here, lines(s)],
            send_sems.at[1],
            plane_sems.at[here, s],
            {"mp": 2 * chip + parity},
        )

    def from_plane(chip, s):
        landed = plane_in.at[chip, lines(s)]
        return push(landed, landed, send_sems.at[1], plane_sems.at[chip, s], other)

    def home(s):
        return push(
            done.at[lines(s)], out.at[lines(s)], send_sems.at[2], out_sems.at[s], mirror
        )

    def pair_sum(chip, s):
        to_pair(chip, s).wait_recv()
        return pair_in[chip, lines(s)].astype(jnp.float32) + own_part(chip, parity, s)[...].astype(
            jnp.float32
        )

    for s in range(PIECES):

        def give(j, carry, s=s):
            to_pair(lax.rem(here + j, chips), s).start()
            return carry

        lax.fori_loop(1, chips + 1, give, 0)

    for s in range(PIECES):

        def pass_on(j, carry, s=s):
            chip = lax.rem(here + j, chips)
            pair_in[chip, lines(s)] = pair_sum(chip, s).astype(jnp.bfloat16)
            to_plane(chip, s).start()
            return carry

        lax.fori_loop(1, chips, pass_on, 0)

    for s in range(PIECES):

        def add(j, total, s=s):
            chip = lax.rem(here + j, chips)
            from_plane(chip, s).wait_recv()
            return total + plane_in[chip, lines(s)].astype(jnp.float32)

        total = pair_sum(here, s)
        for j in range(1, chips):
            total = add(j, total)
        done[lines(s)] = total.astype(jnp.bfloat16)

        @pl.when(jnp.logical_not(alone))
        def _(s=s):
            home(s).start()

    @pl.when(alone)
    def _():
        out[...] = done[...]

    @pl.when(jnp.logical_not(alone))
    def _():
        for s in range(PIECES):
            home(s).wait_recv()
        push(done, done, send_sems.at[2], out_sems.at[0], mirror).wait_send()

    push(pair_in, pair_in, send_sems.at[0], out_sems.at[0], other).wait_send()
    passed = plane_in.at[pl.ds(0, chips - 1)]
    push(passed, passed, send_sems.at[1], out_sems.at[0], other).wait_send()


def sum_of(n, parts):
    members, rows, width = parts.shape
    chips = members // 2
    vmem = pl.BlockSpec(memory_space=pltpu.VMEM)
    return pl.pallas_call(
        functools.partial(scatter_kernel, n, members // n),
        out_shape=jax.ShapeDtypeStruct((rows, width), jnp.bfloat16),
        in_specs=[vmem],
        out_specs=vmem,
        scratch_shapes=[
            pltpu.VMEM((chips, rows, width), jnp.bfloat16),
            pltpu.VMEM((chips, rows, width), jnp.bfloat16),
            pltpu.VMEM((rows, width), jnp.bfloat16),
            pltpu.SemaphoreType.DMA((3,)),
            pltpu.SemaphoreType.DMA((chips, PIECES)),
            pltpu.SemaphoreType.DMA((chips, PIECES)),
            pltpu.SemaphoreType.DMA((PIECES,)),
        ],
        compiler_params=pltpu.CompilerParams(
            collective_id=2, has_side_effects=True, vmem_limit_bytes=40 * 1024 * 1024
        ),
    )(parts)


def per_device(
    patches,
    embed_weight,
    embed_bias,
    pos_embed,
    norm_gain,
    inner_weight,
    inner_bias,
    outer_weight,
    outer_bias,
):
    n_dp = lax.axis_size("dp")
    n_mp = lax.axis_size("mp")
    ratio = n_mp // n_dp
    group_rows = patches.shape[1] * n_mp
    width = embed_weight.shape[1]
    model_width = width * n_mp
    n_positions = pos_embed.shape[0]
    first_row = lax.axis_index("dp") * group_rows
    positions = (first_row + jnp.arange(group_rows, dtype=jnp.int32)) % n_positions
    selector = (positions[:, None] == jnp.arange(n_positions, dtype=jnp.int32)[None, :]).astype(
        jnp.bfloat16
    )
    all_patches = lax.all_gather(patches, "mp", axis=1, tiled=True)
    product = contract_first(all_patches, embed_weight)
    residual = product + embed_bias[None, :]
    residual = residual + jnp.dot(selector, pos_embed, preferred_element_type=jnp.float32)
    row_total = lax.psum(jnp.sum(residual, axis=1), "mp")
    row_mean = row_total / model_width
    centred = residual - row_mean[:, None]
    row_var = lax.psum(jnp.sum(centred * centred, axis=1), "mp") / model_width
    normed = (centred * lax.rsqrt(row_var + norm_eps)[:, None] * norm_gain[None, :]).astype(
        jnp.bfloat16
    )

    blocks = blocks_of(n_dp, n_mp, normed).reshape(ratio, n_dp * group_rows, width)
    preact_part = 0.0
    for b in range(ratio):
        preact_part = preact_part + jnp.dot(
            blocks[b],
            inner_weight[b * width : (b + 1) * width],
            preferred_element_type=jnp.float32,
        )
    all_hidden = hidden_of(n_dp, preact_part.astype(jnp.bfloat16), inner_bias[None, :])
    partials = [
        jnp.dot(
            all_hidden,
            outer_weight[:, b * width : (b + 1) * width],
            preferred_element_type=jnp.float32,
        ).astype(jnp.bfloat16)
        for b in range(ratio)
    ]
    parts = jnp.stack(partials).reshape(n_mp, group_rows, width)
    mlp_out = sum_of(n_dp, parts).astype(jnp.float32)
    return residual + mlp_out + outer_bias[None, :]


def solution(mesh):
    placed = (
        P(None, ("dp", "mp")),
        P(None, "mp"),
        P("mp"),
        P(None, "mp"),
        P("mp"),
        P("dp", "mp"),
        P("mp"),
        P("mp", "dp"),
        P("mp"),
    )
    return jax.shard_map(
        per_device, mesh=mesh, in_specs=placed, out_specs=P("dp", "mp"), check_vma=False
    )
```
